256 devices in a mesh: dp: 8 (over z), mp: 32 (over x, y, core).
Axes of the slice: x: 4, y: 4, z: 8, core: 2. Of those that a mesh axis runs over, the one named last changes fastest.
Arguments:
- activations: bfloat16 [12288, 8192], P('dp', 'mp'), may hold values from -6 to 6
- grad_output: bfloat16 [12288, 16384], P('dp', 'mp'), may hold values from -0.0546875 to 0.0546875
- holder_index: int32 [32, 32, 1], replicated, may hold values from 0 to 31; in each aligned block of 32 rows (0 to 31, 32 to 63, ..., all dimensions but the last counted through in order) no two rows name the same one
- row_offset: int32 [32, 32], replicated, may hold values from 0 to 1
- column_offset: int32 [32, 32], replicated, may hold values from 0 to 3
- live_counts: int32 [32], replicated, may hold values from 1 to 32, as said below
Outputs:
- candidate_grads: float32 [32, 32, 128, 128], P('mp', 'dp')
The draws below stay inside these ranges and needn't reach their ends.
Inputs may be any that keep to these rules, and one draw needn't show every extreme that they name: In each owner's 32 slots at most 1 have the same holder_index, a bound that some block reaches. Slots from live_counts[o] on are unused; some owner uses all 32 slots.
All inputs are finite; a program needn't handle non-finite values.
Results may differ from the reference program's by a relative error of at most 0.0003.
Values may be sent and summed in bfloat16 or wider, within the bound.
A program may use at most 192 MiB of HBM per device.

```python
import math
import jax
import jax.numpy as jnp
import numpy as np
from jax import lax

D = 8192
FFW = 16384
BLK = 128
CAND = 32
OWNERS = 32
TOKENS = 12288
PER_PEER = 1


def draw_live_counts(key, part):
    first_key, second_key = jax.random.split(jax.random.fold_in(key, 7))
    counted = jax.random.randint(first_key, (OWNERS,), 1, CAND + 1)
    fullest = jax.random.randint(second_key, (), 0, OWNERS)
    return jnp.where(jnp.arange(OWNERS) == fullest, CAND, counted).astype(jnp.int32)


def plant(entries, own_key, low, high):
    longest = entries.shape.index(max(entries.shape))
    spots = []
    for shift in (0, 1):
        where = [jax.random.randint(jax.random.fold_in(own_key, axis), (), 0, length) for axis, length in enumerate(entries.shape)]
        where[longest] = (where[longest] + shift) % entries.shape[longest]
        spots.append(tuple(where))
    return entries.at[spots[0]].set(low).at[spots[1]].set(high)


def level_of(rng, dims, pieces, smallest, top_value):
    def one(dim, shards_of):
        steps = jax.random.uniform(jax.random.fold_in(jax.random.fold_in(rng, 6), dim), (shards_of,), jnp.float32, smallest / len(pieces), top_value / len(pieces))
        return jnp.repeat(jnp.exp(steps), dims[dim] // shards_of).reshape((-1,) + (1,) * (len(dims) - dim - 1))

    loudness = one(*pieces[0])
    for cut in pieces[1:]:
        loudness = loudness * one(*cut)
    return loudness


def shared_out(own_key, own, number, rows, count, top, reach, lean):
    order = jax.random.permutation(own_key, count)
    heavy_load, ordinary = shares(count, rows * top, reach, lean, True), shares(count, rows * top, reach, lean, False)
    places = jnp.arange(count)

    def named(sizes, offset_by):
        used = int((sizes > 0).sum())
        fixed = max(1, used // 4)
        shifted = fixed + (places - fixed + offset_by * (used - fixed)) % max(1, count - fixed)
        return jnp.zeros((count,), jnp.int32).at[order[jnp.where(places < fixed, places, shifted)]].set(jnp.asarray(sizes, jnp.int32))

    sizes = jnp.where(number % 4 == 0, named(heavy_load, number // 4), named(ordinary, number - number // 4 - 1))
    mixed = jax.random.permutation(jax.random.fold_in(own, 3), count)
    donor, sink = mixed[0:count // 2 * 2:2], mixed[1:count // 2 * 2:2]
    margin = jnp.minimum(sizes[donor] - 1, reach - sizes[sink]) // 2
    margin = jnp.where((donor == order[0]) | (sink == order[0]) | (sizes[sink] == 0), 0, jnp.maximum(margin, 0))
    shifted = jax.random.randint(jax.random.fold_in(own, 4), (count // 2,), 0, 1 << 20) % (margin + 1)
    sizes = sizes.at[donor].add(-shifted).at[sink].add(shifted)
    items = jnp.searchsorted(jnp.cumsum(sizes), jnp.arange(rows * top), side="right").astype(jnp.int32)
    listing = items.reshape(top, rows).T
    listing = listing[jax.random.permutation(jax.random.fold_in(own, 1), rows)]
    offset_by = jax.random.randint(jax.random.fold_in(own, 2), (rows, 1), 0, top)
    return jnp.take_along_axis(listing, (jnp.arange(top)[None, :] + offset_by) % top, axis=1)


def shares(number_of, total, limit, slope, full):
    portions = [(1 << 20) // math.isqrt(rank ** slope) + 1 for rank in range(1, number_of + 1)]
    largest = limit if full else min(limit, max(-(-total // number_of), total * portions[0] // sum(portions)))
    least = 1 if total - largest >= number_of - 1 else 0
    counts, surplus = [largest] + [least] * (number_of - 1), total - largest - least * (number_of - 1)
    while surplus > 0:
        free = [i for i in range(1, number_of) if counts[i] < largest] or [i for i in range(1, number_of) if counts[i] < limit]
        pool, remaining = sum([portions[i] for i in free]), surplus
        for i in free:
            extra = min(limit - counts[i], max(1, remaining * portions[i] // pool), surplus)
            counts[i] = counts[i] + extra
            surplus = surplus - extra
    return np.array(counts)


def gaussian(stream_key, dims, spread, limit, shards=(), held_as=jnp.bfloat16):
    array = jax.random.normal(stream_key, dims, jnp.float32) * spread
    if len(shards) > 0:
        array = level_of(stream_key, dims, shards, -0.22, 0.18) * array
    return jnp.clip(array, min=-limit, max=limit).astype(held_as)


def setup_inputs(seed: int = 0) -> dict:
    seeds = jax.random.split(jax.random.key(seed), 7)
    activations = gaussian(seeds[0], (TOKENS, D), 1.0, 6.0, ((0, 8), (1, 32)))
    grad_output = gaussian(seeds[1], (TOKENS, FFW), TOKENS ** -0.5, 0.0546875, ((0, 8), (1, 32)))
    holder_index_keys = jax.random.split(jax.random.fold_in(seeds[2], 1), OWNERS * CAND // CAND)
    holder_index_turns = jax.random.permutation(jax.random.fold_in(seeds[2], 3), OWNERS * CAND // CAND)
    holder_index = jax.vmap(lambda own, number: shared_out(jax.random.fold_in(seeds[2], 2), own, number, CAND, OWNERS, 1, PER_PEER, 2))(holder_index_keys, holder_index_turns).reshape((OWNERS, CAND, 1))
    row_offset = plant(jax.random.randint(seeds[3], (OWNERS, CAND), 0, D // (OWNERS * BLK)), jax.random.fold_in(seeds[3], 1), 0, (D // (OWNERS * BLK)) - 1).astype(jnp.int32)
    column_offset = plant(jax.random.randint(seeds[4], (OWNERS, CAND), 0, FFW // (OWNERS * BLK)), jax.random.fold_in(seeds[4], 1), 0, (FFW // (OWNERS * BLK)) - 1).astype(jnp.int32)
    live_counts = draw_live_counts(jax.random.fold_in(seeds[6], 71), 0)
    return {"activations": activations, "grad_output": grad_output, "holder_index": holder_index, "row_offset": row_offset, "column_offset": column_offset, "live_counts": live_counts}


def reference(activations, grad_output, holder_index, row_offset, column_offset, live_counts):
    per_holder = D // (OWNERS * BLK)
    per_owner = FFW // (OWNERS * BLK)
    row_ids = (holder_index[:, :, 0] * per_holder + row_offset).astype(jnp.int32)
    column_ids = (jnp.arange(OWNERS, dtype=jnp.int32)[:, None] * per_owner + column_offset).astype(jnp.int32)
    input_panels = activations.reshape(activations.shape[0], D // BLK, BLK)
    grad_panels = grad_output.reshape(grad_output.shape[0], FFW // BLK, BLK)
    is_used = jnp.arange(CAND, dtype=jnp.int32)[None, :] < live_counts[:, None]

    def one_owner(packed):
        rows_here, columns_here, used_here = packed
        picked_input = jnp.take(input_panels, rows_here, axis=1).astype(jnp.float32)
        picked_grad = jnp.take(grad_panels, columns_here, axis=1).astype(jnp.float32)
        blocks = jnp.einsum("tkr,tkc->krc", picked_input, picked_grad, precision=lax.Precision.HIGHEST)
        return jnp.where(used_here[:, None, None], blocks, jnp.zeros_like(blocks))

    return lax.map(one_owner, (row_ids, column_ids, is_used))
```

```python
import jax
import jax.numpy as jnp
from jax import lax
from jax.experimental import pallas as pl
from jax.experimental.pallas import tpu as pltpu
from jax.sharding import PartitionSpec as P

BLK = 128
SIDE = 4
RING = 8
CHUNKS = 6
MESH = pl.DeviceIdType.MESH
SIGNS = (1, -1)
PLACE = {0: 0, -1: 1, 1: 2, 2: 3}
LAST = CHUNKS - 1


def kernel(meta, a_hbm, g_hbm, out, *scratch):
    bufs = scratch[:CHUNKS]
    (acc, graw, gt, zrecv, a_sem, g_sem, p1_s, p1_r, q1_s, q1_r, p2_s, p2_r, q2_s, q2_r,
     sib_s, sib_r, z_s, z_r) = scratch[CHUNKS:]
    step = bufs[0].shape[1]
    me = lax.axis_index("mp")
    z = lax.axis_index("dp")
    core = me % 2
    y = (me // 2) % SIDE
    x = me // (2 * SIDE)

    def near(axis, sign):
        if axis == 0:
            there = (((x + sign + SIDE) % SIDE) * SIDE + y) * 2 + core
        else:
            there = (x * SIDE + (y + sign + SIDE) % SIDE) * 2 + core
        return {"mp": there}

    plane = {(axis, sign): near(axis, sign) for axis in (0, 1) for sign in SIGNS}
    sibling = {"mp": me + 1 - 2 * core}
    above = {sign: {"dp": (z + sign + RING) % RING} for sign in SIGNS}

    def remote(src, dst, send, recv, device):
        return pltpu.make_async_remote_copy(
            src_ref=src, dst_ref=dst, send_sem=send, recv_sem=recv, device_id=device, device_id_type=MESH
        )

    def at(half, rel, second, first, count=1):
        return pl.ds(((half * 2 + rel) * SIDE + second) * SIDE + first, count)

    def first_hop(c, h, sign):
        d = 0 if sign > 0 else 1
        return remote(bufs[c].at[at(h, 0, 0, 0)], bufs[c].at[at(h, 0, 0, PLACE[-sign])],
                      p1_s.at[c, h, d], p1_r.at[c, h, d], plane[h, sign])

    def first_relay(c, h):
        sign = 1 if (c + h) % 2 == 0 else -1
        return remote(bufs[c].at[at(h, 0, 0, PLACE[-sign])], bufs[c].at[at(h, 0, 0, 3)],
                      q1_s.at[c, h], q1_r.at[c, h], plane[h, sign])

    def row_hop(c, h, sign):
        d = 0 if sign > 0 else 1
        return remote(bufs[c].at[at(h, 0, 0, 0, 4)], bufs[c].at[at(h, 0, PLACE[-sign], 0, 4)],
                      p2_s.at[c, h, d], p2_r.at[c, h, d], plane[1 - h, sign])

    def row_relay(c, h, sign):
        d = 0 if sign > 0 else 1
        return remote(bufs[c].at[at(h, 0, PLACE[-sign], 2 * d, 2)], bufs[c].at[at(h, 0, 3, 2 * d, 2)],
                      q2_s.at[c, h, d], q2_r.at[c, h, d], plane[1 - h, sign])

    def share(c, h, piece):
        second, count = (0, 12) if piece == 0 else (3, 4)
        return remote(bufs[c].at[at(h, 0, second, 0, count)], bufs[c].at[at(h, 1, second, 0, count)],
                      sib_s.at[c, h, piece], sib_r.at[c, h, piece], sibling)

    def own(c, h):
        return pltpu.make_async_copy(
            a_hbm.at[pl.ds(c * step, step), pl.ds(h * BLK, BLK)],
            bufs[c].at[h * 32], a_sem.at[c, h])

    def panel(k):
        return pltpu.make_async_copy(g_hbm.at[:, pl.ds(k * BLK, BLK)], graw.at[k], g_sem.at[k])

    for c in range(CHUNKS):
        for h in (0, 1):
            own(c, h).start()
    for k in range(4):
        panel(k).start()

    barrier = pltpu.get_barrier_semaphore()
    peers = list(plane.values()) + [sibling] + list(above.values())
    for peer in peers:
        pl.semaphore_signal(barrier, inc=1, device_id=peer, device_id_type=MESH)
    pl.semaphore_wait(barrier, len(peers))

    for c in range(CHUNKS):
        for h in (0, 1):
            own(c, h).wait()
            for sign in SIGNS:
                first_hop(c, h, sign).start()

    for k in range(4):
        panel(k).wait()

    def turn(n, carry):
        for c in range(CHUNKS):
            gt[n, c] = graw[n, pl.ds(c * step, step), :].T
        return carry

    lax.fori_loop(0, 4, turn, 0)

    def products(c, g):
        base = ((z + g) % RING) * 4
        for i in range(4):
            word = meta[base + i]
            block = bufs[c][(word >> 2) & 63]
            part = jnp.dot(gt[word & 3, c], block, preferred_element_type=jnp.float32)
            if c == 0:
                acc[g, i] = part
            else:
                acc[g, i] += part

    def ring_size(sign, i):
        return 4 if (sign > 0) == (i < 2) else 3

    def z_hop(sign, i, t):
        d = 0 if sign > 0 else 1
        g = (sign * (ring_size(sign, i) - t)) % RING
        return g, remote(acc.at[g, i], zrecv.at[d, i, t], z_s.at[d, i, t], z_r.at[d, i, t], above[sign])

    long_chains = [(1, 0), (-1, 2), (1, 1), (-1, 3)]
    short_chains = [(1, 2), (-1, 0), (1, 3), (-1, 1)]

    for it in range(CHUNKS + 3):
        c = it
        if c < CHUNKS:
            for h in (0, 1):
                for sign in SIGNS:
                    first_hop(c, h, sign).wait_recv()
                first_relay(c, h).start()
            for h in (0, 1):
                first_relay(c, h).wait_recv()
                for sign in SIGNS:
                    row_hop(c, h, sign).start()
        c = it - 1
        if 0 <= c < CHUNKS:
            for h in (0, 1):
                for sign in SIGNS:
                    row_hop(c, h, sign).wait_recv()
                    row_relay(c, h, sign).start()
                share(c, h, 0).start()
        c = it - 2
        if 0 <= c < CHUNKS:
            for h in (0, 1):
                for sign in SIGNS:
                    row_relay(c, h, sign).wait_recv()
                share(c, h, 1).start()
        c = it - 3
        if 0 <= c < CHUNKS:
            for h in (0, 1):
                for piece in (0, 1):
                    share(c, h, piece).wait_recv()
            if c < LAST:
                def group(g, carry, c=c):
                    products(c, g)
                    return carry

                lax.fori_loop(0, RING, group, 0)

    products(LAST, 4)
    for sign, i in long_chains:
        z_hop(sign, i, 0)[1].start()

    def nearer(n, carry):
        products(LAST, 3 + 2 * n)
        return carry

    lax.fori_loop(0, 2, nearer, 0)
    for sign, i in short_chains:
        z_hop(sign, i, 0)[1].start()

    def rest(n, carry):
        products(LAST, (n + 6) % RING)
        return carry

    lax.fori_loop(0, 5, rest, 0)

    for t in range(1, 4):
        for sign, i in long_chains + (short_chains if t < 3 else []):
            d = 0 if sign > 0 else 1
            z_hop(sign, i, t - 1)[1].wait_recv()
            g, hop = z_hop(sign, i, t)
            acc[g, i] += zrecv[d, i, t - 1]
            hop.start()

    for c in range(CHUNKS):
        for h in (0, 1):
            for sign in SIGNS:
                first_hop(c, h, sign).wait_send()
                row_hop(c, h, sign).wait_send()
                row_relay(c, h, sign).wait_send()
            first_relay(c, h).wait_send()
            share(c, h, 0).wait_send()
            share(c, h, 1).wait_send()

    for i in (2, 0, 3, 1):
        total = acc[0, i]
        for sign in ((-1, 1) if i < 2 else (1, -1)):
            d = 0 if sign > 0 else 1
            t = ring_size(sign, i) - 1
            z_hop(sign, i, t)[1].wait_recv()
            total = total + zrecv[d, i, t]
        live = meta[z * 4 + i] >> 8
        out[i] = jnp.where(live > 0, total.T, jnp.zeros_like(total))

    for sign in SIGNS:
        for i in range(4):
            for t in range(ring_size(sign, i)):
                z_hop(sign, i, t)[1].wait_send()


def on_device(activations, grad_output, holder_index, row_offset, column_offset, live_counts):
    tokens, slots = activations.shape[0], row_offset.shape[1]
    step = tokens // CHUNKS
    me = lax.axis_index("mp")
    x, y, core = me >> 3, (me >> 1) & 3, me & 1
    holder = lax.dynamic_index_in_dim(holder_index[:, :, 0], me, 0, keepdims=False)
    half = lax.dynamic_index_in_dim(row_offset, me, 0, keepdims=False)
    column = lax.dynamic_index_in_dim(column_offset, me, 0, keepdims=False)
    count = lax.dynamic_index_in_dim(live_counts, me, 0, keepdims=False)

    def place(there, here):
        gap = (there - here) & 3
        return jnp.where(gap == 3, 1, jnp.where(gap == 0, 0, gap + 1))

    px, py = place(holder >> 3, x), place((holder >> 1) & 3, y)
    rel = (holder & 1) ^ core
    spot = half * 32 + rel * 16 + jnp.where(half == 0, py * 4 + px, px * 4 + py)
    used = (jnp.arange(slots, dtype=jnp.int32) < count).astype(jnp.int32)
    meta = spot * 4 + column + used * 256

    dma = pltpu.SemaphoreType.DMA
    out = pl.pallas_call(
        kernel,
        out_shape=jax.ShapeDtypeStruct((slots // RING, BLK, BLK), jnp.float32),
        in_specs=[
            pl.BlockSpec(memory_space=pltpu.SMEM),
            pl.BlockSpec(memory_space=pl.ANY),
            pl.BlockSpec(memory_space=pl.ANY),
        ],
        out_specs=pl.BlockSpec(memory_space=pltpu.VMEM),
        scratch_shapes=[pltpu.VMEM((64, step, BLK), jnp.bfloat16) for _ in range(CHUNKS)]
        + [
            pltpu.VMEM((RING, 4, BLK, BLK), jnp.float32),
            pltpu.VMEM((4, tokens, BLK), jnp.bfloat16),
            pltpu.VMEM((4, CHUNKS, BLK, step), jnp.bfloat16),
            pltpu.VMEM((2, 4, 4, BLK, BLK), jnp.float32),
            dma((CHUNKS, 2)),
            dma((4,)),
        ]
        + [dma((CHUNKS, 2, 2))] * 2
        + [dma((CHUNKS, 2))] * 2
        + [dma((CHUNKS, 2, 2))] * 6
        + [dma((2, 4, 4))] * 2,
        compiler_params=pltpu.CompilerParams(
            collective_id=0, has_side_effects=True, vmem_limit_bytes=56 * 1024 * 1024
        ),
    )(meta, activations, grad_output)
    return out[None]


def solution(mesh):
    placed = (P("dp", "mp"), P("dp", "mp"), P(), P(), P(), P())
    return jax.shard_map(
        on_device, mesh=mesh, in_specs=placed, out_specs=P("mp", "dp", None, None), check_vma=False
    )
```

```python
import jax
import jax.numpy as jnp
from jax import lax
from jax.experimental import pallas as pl
from jax.experimental.pallas import tpu as pltpu
from jax.sharding import PartitionSpec as P

BLK = 128
SIDE = 4
RING = 8
SIZES = (32, 32, 32, 32)
PIECES = len(SIZES)
STARTS = tuple(sum(SIZES[:p]) for p in range(PIECES))
LAG = 3
TURN = 256
MESH = pl.DeviceIdType.MESH
SIGNS = (1, -1)
PLACE = {0: 0, -1: 1, 1: 2, 2: 3}


def kernel(meta, a_hbm, g_hbm, out, *scratch):
    bufs = scratch[:PIECES]
    accs = scratch[PIECES : 2 * PIECES]
    lands = scratch[2 * PIECES : 3 * PIECES]
    (araw, graw, picked, a_sem, g_sem, p1_s, p1_r, q1_s, q1_r, p2_s, p2_r, q2_s, q2_r,
     sib_s, sib_r, z_s, z_r) = scratch[3 * PIECES :]
    me = lax.axis_index("mp")
    z = lax.axis_index("dp")
    core = me % 2
    y = (me // 2) % SIDE
    x = me // (2 * SIDE)

    def near(axis, sign):
        if axis == 0:
            there = (((x + sign + SIDE) % SIDE) * SIDE + y) * 2 + core
        else:
            there = (x * SIDE + (y + sign + SIDE) % SIDE) * 2 + core
        return {"mp": there}

    plane = {(axis, sign): near(axis, sign) for axis in (0, 1) for sign in SIGNS}
    sibling = {"mp": me + 1 - 2 * core}
    above = {sign: {"dp": (z + sign + RING) % RING} for sign in SIGNS}

    def remote(src, dst, send, recv, device):
        return pltpu.make_async_remote_copy(
            src_ref=src, dst_ref=dst, send_sem=send, recv_sem=recv, device_id=device, device_id_type=MESH
        )

    def at(half, rel, second, first, count=1):
        return pl.ds(((half * 2 + rel) * SIDE + second) * SIDE + first, count)

    def first_hop(p, h, sign):
        d = 0 if sign > 0 else 1
        return remote(bufs[p].at[at(h, 0, 0, 0)], bufs[p].at[at(h, 0, 0, PLACE[-sign])],
                      p1_s.at[p, h, d], p1_r.at[p, h, d], plane[h, sign])

    def first_relay(p, h):
        sign = 1 if (p + h) % 2 == 0 else -1
        return remote(bufs[p].at[at(h, 0, 0, PLACE[-sign])], bufs[p].at[at(h, 0, 0, 3)],
                      q1_s.at[p, h], q1_r.at[p, h], plane[h, sign])

    def row_hop(p, h, q, sign):
        d = 0 if sign > 0 else 1
        return remote(bufs[p].at[at(h, 0, 0, q)], bufs[p].at[at(h, 0, PLACE[-sign], q)],
                      p2_s.at[p, h, q, d], p2_r.at[p, h, q, d], plane[1 - h, sign])

    def row_relay(p, h, q):
        sign = 1 if q % 2 == 0 else -1
        return remote(bufs[p].at[at(h, 0, PLACE[-sign], q)], bufs[p].at[at(h, 0, 3, q)],
                      q2_s.at[p, h, q], q2_r.at[p, h, q], plane[1 - h, sign])

    def share(p, h, part):
        second, count = (0, 12) if part == 0 else (3, 4)
        return remote(bufs[p].at[at(h, 0, second, 0, count)], bufs[p].at[at(h, 1, second, 0, count)],
                      sib_s.at[p, h, part], sib_r.at[p, h, part], sibling)

    load = pltpu.make_async_copy(a_hbm, araw, a_sem)
    load.start()

    panels = pltpu.make_async_copy(g_hbm, graw, g_sem)
    panels.start()

    barrier = pltpu.get_barrier_semaphore()
    peers = list(plane.values()) + [sibling] + list(above.values())
    for peer in peers:
        pl.semaphore_signal(barrier, inc=1, device_id=peer, device_id_type=MESH)

    load.wait()
    for n in range(araw.shape[0] // TURN):
        for h in (0, 1):
            turned = araw[pl.ds(n * TURN, TURN), pl.ds(h * BLK, BLK)].T
            for p in range(PIECES):
                bufs[p][32 * h, :, pl.ds(n * TURN, TURN)] = turned[STARTS[p] : STARTS[p] + SIZES[p], :]

    pl.semaphore_wait(barrier, len(peers))

    for p in range(PIECES):
        for h in (0, 1):
            for sign in SIGNS:
                first_hop(p, h, sign).start()
    for p in range(PIECES):
        for h in (0, 1):
            for sign in SIGNS:
                first_hop(p, h, sign).wait_recv()
            first_relay(p, h).start()
    panels.wait()

    def products(p, n):
        size = SIZES[p]
        groups = (n + 4, 3 - n)
        words = [meta[me, ((z + g) % RING) * 4 + i] for g in groups for i in range(4)]
        for s, word in enumerate(words):
            picked[pl.ds(s * size, size), :] = bufs[p][(word >> 2) & 63]
        every = jnp.dot(picked[: 8 * size, :], graw[...], preferred_element_type=jnp.float32)
        for s, word in enumerate(words):
            part = every[s * size : (s + 1) * size]
            low = jnp.where((word & 1) == 0, part[:, :BLK], part[:, BLK : 2 * BLK])
            high = jnp.where((word & 1) == 0, part[:, 2 * BLK : 3 * BLK], part[:, 3 * BLK :])
            accs[p][groups[s // 4], s % 4] = jnp.where((word & 2) == 0, low, high)

    def hops(sign, u):
        return 4 if (sign > 0) == (u == 0) else 3

    def z_hop(p, sign, u, t):
        d = 0 if sign > 0 else 1
        g = (sign * (hops(sign, u) - t)) % RING
        return g, remote(accs[p].at[g, pl.ds(2 * u, 2)], lands[p].at[d, u, t],
                         z_s.at[p, d, u, t], z_r.at[p, d, u, t], above[sign])

    chains = [(1, 0), (-1, 1), (1, 1), (-1, 0)]

    def first_groups(p):
        for h in (0, 1):
            for part in (0, 1):
                share(p, h, part).wait_recv()

        def group(n, carry):
            products(p, n)
            return carry

        lax.fori_loop(0, 2, group, 0)
        for sign, u in chains:
            z_hop(p, sign, u, 0)[1].start()

    def other_groups(p):
        def group(n, carry):
            products(p, n)
            return carry

        lax.fori_loop(2, 4, group, 0)

    def z_step(p, t):
        for sign, u in chains:
            if t >= hops(sign, u):
                continue
            d = 0 if sign > 0 else 1
            z_hop(p, sign, u, t - 1)[1].wait_recv()
            g, hop = z_hop(p, sign, u, t)
            accs[p][g, pl.ds(2 * u, 2)] += lands[p][d, u, t - 1]
            hop.start()

    def z_end(p):
        for u in (1, 0):
            total = accs[p][0, pl.ds(2 * u, 2)]
            for sign in ((1, -1) if u else (-1, 1)):
                d = 0 if sign > 0 else 1
                t = hops(sign, u) - 1
                z_hop(p, sign, u, t)[1].wait_recv()
                total = total + lands[p][d, u, t]
            for i in (0, 1):
                live = meta[me, z * 4 + 2 * u + i] >> 8
                out[2 * u + i, pl.ds(STARTS[p], SIZES[p]), :] = jnp.where(
                    live > 0, total[i], jnp.zeros_like(total[i])
                )

    blocks = 4 * PIECES
    for k in range(blocks + LAG + 9):
        if k < blocks:
            p, q = k // 4, k % 4
            for h in (0, 1):
                if q == 3:
                    first_relay(p, h).wait_recv()
                for sign in SIGNS:
                    row_hop(p, h, q, sign).start()
        if 0 <= k - LAG < blocks:
            p, q = (k - LAG) // 4, (k - LAG) % 4
            for h in (0, 1):
                for sign in SIGNS:
                    row_hop(p, h, q, sign).wait_recv()
                row_relay(p, h, q).start()
            if q == 3:
                for h in (0, 1):
                    share(p, h, 0).start()
        for p in range(PIECES):
            since = k - (4 * p + 3 + LAG)
            if since == 2:
                for h in (0, 1):
                    for q in range(4):
                        row_relay(p, h, q).wait_recv()
                    share(p, h, 1).start()
            elif since == 3:
                first_groups(p)
            elif since == 4:
                other_groups(p)
            elif 5 <= since <= 7:
                z_step(p, since - 4)
            elif since == 8:
                z_end(p)

    for p in range(PIECES):
        for h in (0, 1):
            for sign in SIGNS:
                first_hop(p, h, sign).wait_send()
                for q in range(4):
                    row_hop(p, h, q, sign).wait_send()
            first_relay(p, h).wait_send()
            for q in range(4):
                row_relay(p, h, q).wait_send()
            for part in (0, 1):
                share(p, h, part).wait_send()
        for sign, u in chains:
            for t in range(hops(sign, u)):
                z_hop(p, sign, u, t)[1].wait_send()


def on_device(activations, grad_output, holder_index, row_offset, column_offset, live_counts):
    tokens, slots = activations.shape[0], row_offset.shape[1]
    mine = lax.broadcasted_iota(jnp.int32, row_offset.shape, 0)
    slot = lax.broadcasted_iota(jnp.int32, row_offset.shape, 1)
    holder = holder_index[:, :, 0]

    def place(gap):
        gap = gap & 3
        return jnp.where(gap == 3, 1, jnp.where(gap == 0, 0, gap + 1))

    px = place((holder >> 3) - (mine >> 3))
    py = place((holder >> 1) - (mine >> 1))
    rel = (holder ^ mine) & 1
    spot = row_offset * 32 + rel * 16 + jnp.where(row_offset == 0, py * 4 + px, px * 4 + py)
    used = (slot < live_counts[:, None]).astype(jnp.int32)
    meta = spot * 4 + column_offset + used * 256

    dma = pltpu.SemaphoreType.DMA
    out = pl.pallas_call(
        kernel,
        out_shape=jax.ShapeDtypeStruct((slots // RING, BLK, BLK), jnp.float32),
        in_specs=[
            pl.BlockSpec(memory_space=pltpu.SMEM),
            pl.BlockSpec(memory_space=pl.ANY),
            pl.BlockSpec(memory_space=pl.ANY),
        ],
        out_specs=pl.BlockSpec(memory_space=pltpu.VMEM),
        scratch_shapes=[pltpu.VMEM((64, size, tokens), jnp.bfloat16) for size in SIZES]
        + [pltpu.VMEM((RING, 4, size, BLK), jnp.float32) for size in SIZES]
        + [pltpu.VMEM((2, 2, 4, 2, size, BLK), jnp.float32) for size in SIZES]
        + [
            pltpu.VMEM(activations.shape, jnp.bfloat16),
            pltpu.VMEM(grad_output.shape, jnp.bfloat16),
            pltpu.VMEM((8 * max(SIZES), tokens), jnp.bfloat16),
            dma,
            dma,
        ]
        + [dma((PIECES, 2, 2))] * 2
        + [dma((PIECES, 2))] * 2
        + [dma((PIECES, 2, 4, 2))] * 2
        + [dma((PIECES, 2, 4))] * 2
        + [dma((PIECES, 2, 2))] * 2
        + [dma((PIECES, 2, 2, 4))] * 2,
        compiler_params=pltpu.CompilerParams(
            collective_id=0, has_side_effects=True, vmem_limit_bytes=56 * 1024 * 1024
        ),
    )(meta, activations, grad_output)
    return out[None]


def solution(mesh):
    placed = (P("dp", "mp"), P("dp", "mp"), P(), P(), P(), P())
    return jax.shard_map(
        on_device, mesh=mesh, in_specs=placed, out_specs=P("mp", "dp", None, None), check_vma=False
    )
```

```python
import jax
import jax.numpy as jnp
from jax import lax
from jax.experimental import pallas as pl
from jax.experimental.pallas import tpu as pltpu
from jax.sharding import PartitionSpec as P

BLK = 128
SIDE = 4
RING = 8
SIZES = (48, 32, 32, 16)
PIECES = len(SIZES)
STARTS = tuple(sum(SIZES[:p]) for p in range(PIECES))
LAG = 96
TURN = 256
MESH = pl.DeviceIdType.MESH
SIGNS = (1, -1)
PLACE = {0: 0, -1: 1, 1: 2, 2: 3}


def kernel(holders, offsets, columns, counts, a_hbm, g_hbm, out, *scratch):
    bufs = scratch[:PIECES]
    accs = scratch[PIECES : 2 * PIECES]
    lands = scratch[2 * PIECES : 3 * PIECES]
    (holder_s, offset_s, column_s, count_s, meta, table_sem, araw, graw, picked, a_sem, g_sem, p1_s, p1_r, q1_s, q1_r, p2_s, p2_r, q2_s, q2_r,
     sib_s, sib_r, z_s, z_r) = scratch[3 * PIECES :]
    me = lax.axis_index("mp")
    z = lax.axis_index("dp")
    core = me % 2
    y = (me // 2) % SIDE
    x = me // (2 * SIDE)

    def near(axis, sign):
        if axis == 0:
            there = (((x + sign + SIDE) % SIDE) * SIDE + y) * 2 + core
        else:
            there = (x * SIDE + (y + sign + SIDE) % SIDE) * 2 + core
        return {"mp": there}

    plane = {(axis, sign): near(axis, sign) for axis in (0, 1) for sign in SIGNS}
    sibling = {"mp": me + 1 - 2 * core}
    above = {step: {"dp": (z + step + RING) % RING} for step in (1, -1, 2, -2)}

    def remote(src, dst, send, recv, device):
        return pltpu.make_async_remote_copy(
            src_ref=src, dst_ref=dst, send_sem=send, recv_sem=recv, device_id=device, device_id_type=MESH
        )

    def at(half, rel, second, first, count=1):
        return pl.ds(((half * 2 + rel) * SIDE + second) * SIDE + first, count)

    def first_hop(p, h, sign):
        d = 0 if sign > 0 else 1
        return remote(bufs[p].at[at(h, 0, 0, 0)], bufs[p].at[at(h, 0, 0, PLACE[-sign])],
                      p1_s.at[p, h, d], p1_r.at[p, h, d], plane[h, sign])

    def first_relay(p, h):
        sign = 1 if (p + h) % 2 == 0 else -1
        return remote(bufs[p].at[at(h, 0, 0, PLACE[-sign])], bufs[p].at[at(h, 0, 0, 3)],
                      q1_s.at[p, h], q1_r.at[p, h], plane[h, sign])

    def row_hop(p, h, q, sign):
        d = 0 if sign > 0 else 1
        return remote(bufs[p].at[at(h, 0, 0, q)], bufs[p].at[at(h, 0, PLACE[-sign], q)],
                      p2_s.at[p, h, q, d], p2_r.at[p, h, q, d], plane[1 - h, sign])

    def row_relay(p, h, q):
        sign = 1 if q % 2 == 0 else -1
        return remote(bufs[p].at[at(h, 0, PLACE[-sign], q)], bufs[p].at[at(h, 0, 3, q)],
                      q2_s.at[p, h, q], q2_r.at[p, h, q], plane[1 - h, sign])

    def share(p, h, part):
        second, count = (0, 12) if part == 0 else (3, 4)
        return remote(bufs[p].at[at(h, 0, second, 0, count)], bufs[p].at[at(h, 1, second, 0, count)],
                      sib_s.at[p, h, part], sib_r.at[p, h, part], sibling)

    load = pltpu.make_async_copy(a_hbm, araw, a_sem)
    load.start()

    panels = pltpu.make_async_copy(g_hbm, graw, g_sem)
    panels.start()
    tables = [
        pltpu.make_async_copy(src, dst, table_sem.at[n])
        for n, (src, dst) in enumerate(
            ((holders.at[me], holder_s), (offsets, offset_s), (columns, column_s), (counts, count_s))
        )
    ]
    for table in tables:
        table.start()

    barrier = pltpu.get_barrier_semaphore()
    peers = list(plane.values()) + [sibling] + list(above.values())
    for peer in peers:
        pl.semaphore_signal(barrier, inc=1, device_id=peer, device_id_type=MESH)

    load.wait()
    for n in range(araw.shape[0] // TURN):
        for h in (0, 1):
            turned = araw[pl.ds(n * TURN, TURN), pl.ds(h * BLK, BLK)].T
            for p in range(PIECES):
                bufs[p][32 * h, :, pl.ds(n * TURN, TURN)] = turned[STARTS[p] : STARTS[p] + SIZES[p], :]

    pl.semaphore_wait(barrier, len(peers))

    for p in range(PIECES):
        for h in (0, 1):
            for sign in SIGNS:
                first_hop(p, h, sign).start()
    for p in range(PIECES):
        for h in (0, 1):
            for sign in SIGNS:
                first_hop(p, h, sign).wait_recv()
            first_relay(p, h).start()
    panels.wait()
    for table in tables:
        table.wait()

    def place(gap):
        gap = gap & 3
        return jnp.where(gap == 3, 1, jnp.where(gap == 0, 0, gap + 1))

    def note(j, carry):
        holder, half = holder_s[0, j], offset_s[me, j]
        px, py = place((holder >> 3) - x), place(((holder >> 1) & 3) - y)
        spot = half * 32 + ((holder ^ core) & 1) * 16 + jnp.where(half == 0, py * 4 + px, px * 4 + py)
        meta[j] = spot * 4 + column_s[me, j] + jnp.where(j < count_s[me], 256, 0)
        return carry

    lax.fori_loop(0, 32, note, 0)

    def products(p, n):
        size = SIZES[p]
        groups = (n + 4, 3 - n)
        words = [meta[((z + g) % RING) * 4 + i] for g in groups for i in range(4)]
        for s, word in enumerate(words):
            picked[pl.ds(s * size, size), :] = bufs[p][(word >> 2) & 63]
        every = jnp.dot(picked[: 8 * size, :], graw[...], preferred_element_type=jnp.float32)
        for s, word in enumerate(words):
            part = every[s * size : (s + 1) * size]
            low = jnp.where((word & 1) == 0, part[:, :BLK], part[:, BLK : 2 * BLK])
            high = jnp.where((word & 1) == 0, part[:, 2 * BLK : 3 * BLK], part[:, 3 * BLK :])
            accs[p][groups[s // 4], s % 4] = jnp.where((word & 2) == 0, low, high)

    def leaf(p, name):
        acc, land = accs[p], lands[p]
        src, dst, step, n = {
            "far_up": (acc.at[4, pl.ds(0, 2)], land.at[0, pl.ds(0, 2)], 2, 0),
            "far_down": (acc.at[4, pl.ds(2, 2)], land.at[0, pl.ds(2, 2)], -2, 1),
            "third_up": (acc.at[3], land.at[1], 1, 2),
            "third_down": (acc.at[5], land.at[2], -1, 3),
            "next_up": (acc.at[1], land.at[3], 1, 4),
            "next_down": (acc.at[7], land.at[4], -1, 5),
            "sum_up": (acc.at[2], land.at[5], 2, 6),
            "sum_down": (acc.at[6], land.at[6], -2, 7),
        }[name]
        return remote(src, dst, z_s.at[p, n], z_r.at[p, n], above[step])

    names = ("far_up", "far_down", "third_up", "third_down", "next_up", "next_down", "sum_up", "sum_down")

    def ready(p):
        for h in (0, 1):
            for q in range(4):
                row_relay(p, h, q).wait_recv()
            share(p, h, 1).start()

    def first_groups(p):
        for h in (0, 1):
            for part in (0, 1):
                share(p, h, part).wait_recv()

        def group(n, carry):
            products(p, n)
            return carry

        lax.fori_loop(0, 2, group, 0)
        for name in names[:4]:
            leaf(p, name).start()

    def other_groups(p):
        def group(n, carry):
            products(p, n)
            return carry

        lax.fori_loop(2, 4, group, 0)
        for name in names[4:6]:
            leaf(p, name).start()

    def gather(p):
        acc, land = accs[p], lands[p]
        for name in names[:4]:
            leaf(p, name).wait_recv()
        acc[2] += land[1]
        acc[2, pl.ds(0, 2)] += land[0, pl.ds(0, 2)]
        acc[6] += land[2]
        acc[6, pl.ds(2, 2)] += land[0, pl.ds(2, 2)]
        leaf(p, "sum_up").start()
        leaf(p, "sum_down").start()

    def finish(p):
        for name in names[4:]:
            leaf(p, name).wait_recv()
        land = lands[p]
        total = accs[p][0] + ((land[3] + land[4]) + (land[5] + land[6]))
        for i in range(4):
            live = meta[z * 4 + i] >> 8
            out[i, pl.ds(STARTS[p], SIZES[p]), :] = jnp.where(live > 0, total[i], jnp.zeros_like(total[i]))

    order = [(p, q) for p in range(PIECES) for q in range(4)]
    stages = (ready, first_groups, other_groups, gather, finish)
    due = []
    for p in range(PIECES):
        after = SIZES[min(p + 1, PIECES - 1)]
        waits = (2, 3, 4, 6, 8) if after > 16 or p == PIECES - 1 else (3, 5, 6, 9, 11)
        due += [(4 * p + 3 + wait, p, stage) for wait, stage in zip(waits, stages)]
    due.sort(key=lambda entry: entry[:2])

    def sends(p, n):
        return {1: (0, 2, 1, 3)[n], -1: (1, 3, 0, 2)[n]} if p else {1: n, -1: n}

    def pass_on(k):
        p, n = order[k]
        for h in (0, 1):
            for sign, q in sends(p, n).items():
                row_hop(p, h, q, sign).wait_recv()
                if (q % 2 == 0) == (sign > 0):
                    row_relay(p, h, q).start()
        if n == 3:
            for h in (0, 1):
                share(p, h, 0).start()
        while due and due[0][0] <= k:
            _, p, stage = due.pop(0)
            stage(p)

    behind = passed = 0
    for p, n in order:
        for h in (0, 1):
            if n == (1 if p else 3):
                first_relay(p, h).wait_recv()
            for sign, q in sends(p, n).items():
                row_hop(p, h, q, sign).start()
        behind += SIZES[p]
        while behind - SIZES[order[passed][0]] >= LAG:
            behind -= SIZES[order[passed][0]]
            pass_on(passed)
            passed += 1
    for k in range(passed, len(order)):
        pass_on(k)

    def settle():
        for p in range(PIECES):
            for h in (0, 1):
                for sign in SIGNS:
                    first_hop(p, h, sign).wait_send()
                    for q in range(4):
                        row_hop(p, h, q, sign).wait_send()
                first_relay(p, h).wait_send()
                for q in range(4):
                    row_relay(p, h, q).wait_send()
                for part in (0, 1):
                    share(p, h, part).wait_send()

    for _, p, stage in due:
        stage(p)
        if p == PIECES - 1 and stage is other_groups:
            settle()
    for p in range(PIECES):
        for name in names:
            leaf(p, name).wait_send()


def on_device(activations, grad_output, holder_index, row_offset, column_offset, live_counts):
    tokens, slots = activations.shape[0], row_offset.shape[1]
    dma = pltpu.SemaphoreType.DMA
    out = pl.pallas_call(
        kernel,
        out_shape=pltpu.VMEM((slots // RING, BLK, BLK), jnp.float32),
        in_specs=[pl.BlockSpec(memory_space=pl.ANY)] * 6,
        out_specs=pl.BlockSpec(memory_space=pltpu.VMEM),
        scratch_shapes=[pltpu.VMEM((64, size, tokens), jnp.bfloat16) for size in SIZES]
        + [pltpu.VMEM((RING, 4, size, BLK), jnp.float32) for size in SIZES]
        + [pltpu.VMEM((7, 4, size, BLK), jnp.float32) for size in SIZES]
        + [
            pltpu.SMEM((1, slots), jnp.int32),
            pltpu.SMEM(row_offset.shape, jnp.int32),
            pltpu.SMEM(row_offset.shape, jnp.int32),
            pltpu.SMEM(live_counts.shape, jnp.int32),
            pltpu.SMEM((slots,), jnp.int32),
            dma((4,)),
            pltpu.VMEM(activations.shape, jnp.bfloat16),
            pltpu.VMEM(grad_output.shape, jnp.bfloat16),
            pltpu.VMEM((8 * max(SIZES), tokens), jnp.bfloat16),
            dma,
            dma,
        ]
        + [dma((PIECES, 2, 2))] * 2
        + [dma((PIECES, 2))] * 2
        + [dma((PIECES, 2, 4, 2))] * 2
        + [dma((PIECES, 2, 4))] * 2
        + [dma((PIECES, 2, 2))] * 2
        + [dma((PIECES, 8))] * 2,
        compiler_params=pltpu.CompilerParams(
            collective_id=0, has_side_effects=True, vmem_limit_bytes=56 * 1024 * 1024
        ),
    )(holder_index.transpose(0, 2, 1), row_offset, column_offset, live_counts, activations, grad_output)
    return out[None]


def solution(mesh):
    placed = (P("dp", "mp"), P("dp", "mp"), P(), P(), P(), P())
    return jax.shard_map(
        on_device, mesh=mesh, in_specs=placed, out_specs=P("mp", "dp", None, None), check_vma=False
    )
```

```python
import jax
import jax.numpy as jnp
from jax import lax
from jax.experimental import pallas as pl
from jax.experimental.pallas import tpu as pltpu
from jax.sharding import PartitionSpec as P

BLK = 128
SIDE = 4
RING = 8
SIZES = (48, 32, 32, 16)
PIECES = len(SIZES)
STARTS = tuple(sum(SIZES[:p]) for p in range(PIECES))
LAG = 96
TURN = 256
MESH = pl.DeviceIdType.MESH
SIGNS = (1, -1)
PLACE = {0: 0, -1: 1, 1: 2, 2: 3}


def kernel(holders, offsets, columns, counts, a_hbm, g_hbm, out, *scratch):
    bufs = scratch[:PIECES]
    accs = scratch[PIECES : 2 * PIECES]
    lands = scratch[2 * PIECES : 3 * PIECES]
    (holder_s, offset_s, column_s, count_s, meta, table_sem, araw, graw, picked, a_sem, g_sem, p1_s, p1_r, q1_s, q1_r, p2_s, p2_r, q2_s, q2_r,
     sib_s, sib_r, z_s, z_r) = scratch[3 * PIECES :]
    me = lax.axis_index("mp")
    z = lax.axis_index("dp")
    core = me % 2
    y = (me // 2) % SIDE
    x = me // (2 * SIDE)

    def near(axis, sign):
        if axis == 0:
            there = (((x + sign + SIDE) % SIDE) * SIDE + y) * 2 + core
        else:
            there = (x * SIDE + (y + sign + SIDE) % SIDE) * 2 + core
        return {"mp": there}

    plane = {(axis, sign): near(axis, sign) for axis in (0, 1) for sign in SIGNS}
    sibling = {"mp": me + 1 - 2 * core}
    above = {step: {"dp": (z + step + RING) % RING} for step in (1, -1, 2, -2)}

    def remote(src, dst, send, recv, device):
        return pltpu.make_async_remote_copy(
            src_ref=src, dst_ref=dst, send_sem=send, recv_sem=recv, device_id=device, device_id_type=MESH
        )

    def at(half, rel, second, first, count=1):
        return pl.ds(((half * 2 + rel) * SIDE + second) * SIDE + first, count)

    def first_hop(p, h, sign):
        d = 0 if sign > 0 else 1
        return remote(bufs[p].at[at(h, 0, 0, 0)], bufs[p].at[at(h, 0, 0, PLACE[-sign])],
                      p1_s.at[p, h, d], p1_r.at[p, h, d], plane[h, sign])

    def first_relay(p, h):
        sign = 1 if (p + h) % 2 == 0 else -1
        return remote(bufs[p].at[at(h, 0, 0, PLACE[-sign])], bufs[p].at[at(h, 0, 0, 3)],
                      q1_s.at[p, h], q1_r.at[p, h], plane[h, sign])

    def row_hop(p, h, q, sign):
        d = 0 if sign > 0 else 1
        return remote(bufs[p].at[at(h, 0, 0, q)], bufs[p].at[at(h, 0, PLACE[-sign], q)],
                      p2_s.at[p, h, q, d], p2_r.at[p, h, q, d], plane[1 - h, sign])

    def row_relay(p, h, q):
        sign = 1 if q % 2 == 0 else -1
        return remote(bufs[p].at[at(h, 0, PLACE[-sign], q)], bufs[p].at[at(h, 0, 3, q)],
                      q2_s.at[p, h, q], q2_r.at[p, h, q], plane[1 - h, sign])

    def share(p, h, part):
        second, count = (0, 12) if part == 0 else (3, 4)
        return remote(bufs[p].at[at(h, 0, second, 0, count)], bufs[p].at[at(h, 1, second, 0, count)],
                      sib_s.at[p, h, part], sib_r.at[p, h, part], sibling)

    load = pltpu.make_async_copy(a_hbm, araw, a_sem)
    load.start()

    panels = pltpu.make_async_copy(g_hbm, graw, g_sem)
    panels.start()
    tables = [
        pltpu.make_async_copy(src, dst, table_sem.at[n])
        for n, (src, dst) in enumerate(
            ((holders.at[me], holder_s), (offsets, offset_s), (columns, column_s), (counts, count_s))
        )
    ]
    for table in tables:
        table.start()

    barrier = pltpu.get_barrier_semaphore()
    peers = list(plane.values()) + [sibling] + list(above.values())
    for peer in peers:
        pl.semaphore_signal(barrier, inc=1, device_id=peer, device_id_type=MESH)

    load.wait()
    for n in range(araw.shape[0] // TURN):
        for h in (0, 1):
            turned = araw[pl.ds(n * TURN, TURN), pl.ds(h * BLK, BLK)].T
            for p in range(PIECES):
                bufs[p][32 * h, :, pl.ds(n * TURN, TURN)] = turned[STARTS[p] : STARTS[p] + SIZES[p], :]

    pl.semaphore_wait(barrier, len(peers))

    for p in range(PIECES):
        for h in (0, 1):
            for sign in SIGNS:
                first_hop(p, h, sign).start()
    for p in range(PIECES):
        for h in (0, 1):
            for sign in SIGNS:
                first_hop(p, h, sign).wait_recv()
            first_relay(p, h).start()
    panels.wait()
    for table in tables:
        table.wait()

    def place(gap):
        gap = gap & 3
        return jnp.where(gap == 3, 1, jnp.where(gap == 0, 0, gap + 1))

    def note(j, carry):
        holder, half = holder_s[0, j], offset_s[me, j]
        px, py = place((holder >> 3) - x), place(((holder >> 1) & 3) - y)
        spot = half * 32 + ((holder ^ core) & 1) * 16 + jnp.where(half == 0, py * 4 + px, px * 4 + py)
        meta[j] = spot * 4 + column_s[me, j] + jnp.where(j < count_s[me], 256, 0)
        return carry

    lax.fori_loop(0, 32, note, 0)

    def products(p, n):
        size = SIZES[p]
        groups = (n + 4, 3 - n)
        words = [meta[((z + g) % RING) * 4 + i] for g in groups for i in range(4)]
        for s, word in enumerate(words):
            picked[pl.ds(s * size, size), :] = bufs[p][(word >> 2) & 63]
        every = jnp.dot(picked[: 8 * size, :], graw[...], preferred_element_type=jnp.float32)
        for s, word in enumerate(words):
            part = every[s * size : (s + 1) * size]
            low = jnp.where((word & 1) == 0, part[:, :BLK], part[:, BLK : 2 * BLK])
            high = jnp.where((word & 1) == 0, part[:, 2 * BLK : 3 * BLK], part[:, 3 * BLK :])
            accs[p][groups[s // 4], s % 4] = jnp.where((word & 2) == 0, low, high)

    def leaf(p, name):
        acc, land = accs[p], lands[p]
        src, dst, step, n = {
            "far_up": (acc.at[4, pl.ds(0, 2)], land.at[0, pl.ds(0, 2)], 2, 0),
            "far_down": (acc.at[4, pl.ds(2, 2)], land.at[0, pl.ds(2, 2)], -2, 1),
            "third_up": (acc.at[3], land.at[1], 1, 2),
            "third_down": (acc.at[5], land.at[2], -1, 3),
            "next_up": (acc.at[1], land.at[3], 1, 4),
            "next_down": (acc.at[7], land.at[4], -1, 5),
            "sum_up": (acc.at[2], land.at[5], 2, 6),
            "sum_down": (acc.at[6], land.at[6], -2, 7),
        }[name]
        return remote(src, dst, z_s.at[p, n], z_r.at[p, n], above[step])

    names = ("far_up", "far_down", "third_up", "third_down", "next_up", "next_down", "sum_up", "sum_down")

    def ready(p):
        for h in (0, 1):
            for q in range(4):
                row_relay(p, h, q).wait_recv()
            share(p, h, 1).start()

    def first_groups(p):
        for h in (0, 1):
            for part in (0, 1):
                share(p, h, part).wait_recv()

        def group(n, carry):
            products(p, n)
            return carry

        lax.fori_loop(0, 2, group, 0)
        for name in names[:4]:
            leaf(p, name).start()

    def other_groups(p):
        def group(n, carry):
            products(p, n)
            return carry

        lax.fori_loop(2, 4, group, 0)
        for name in names[4:6]:
            leaf(p, name).start()

    def gather(p):
        acc, land = accs[p], lands[p]
        for name in names[:4]:
            leaf(p, name).wait_recv()
        acc[2] += land[1]
        acc[2, pl.ds(0, 2)] += land[0, pl.ds(0, 2)]
        acc[6] += land[2]
        acc[6, pl.ds(2, 2)] += land[0, pl.ds(2, 2)]
        leaf(p, "sum_up").start()
        leaf(p, "sum_down").start()

    def finish(p):
        for name in names[4:]:
            leaf(p, name).wait_recv()
        land = lands[p]
        total = accs[p][0] + ((land[3] + land[4]) + (land[5] + land[6]))
        for i in range(4):
            live = meta[z * 4 + i] >> 8
            out[i, pl.ds(STARTS[p], SIZES[p]), :] = jnp.where(live > 0, total[i], jnp.zeros_like(total[i]))

    order = [(p, q) for p in range(PIECES) for q in range(4)]
    stages = (ready, first_groups, other_groups, gather, finish)
    due = []
    for p in range(PIECES):
        after = SIZES[min(p + 1, PIECES - 1)]
        waits = (2, 3, 4, 6, 8)
        if p < PIECES - 1:
            waits = (2, 4, 5, 8, 10) if after == 16 else (1, 2, 3, 5, 7)
        if p == 0:
            waits = (1, 2, 3, 5, 7)
        due += [(4 * p + 3 + wait, p, stage) for wait, stage in zip(waits, stages)]
    due.sort(key=lambda entry: entry[:2])

    def sends(p, n):
        return {1: (0, 2, 1, 3)[n], -1: (1, 3, 0, 2)[n]} if p else {1: n, -1: n}

    def pass_on(k):
        p, n = order[k]
        for h in (0, 1):
            for sign, q in sends(p, n).items():
                row_hop(p, h, q, sign).wait_recv()
                if (q % 2 == 0) == (sign > 0):
                    row_relay(p, h, q).start()
        if n == 3:
            for h in (0, 1):
                share(p, h, 0).start()
        while due and due[0][0] <= k:
            _, p, stage = due.pop(0)
            stage(p)

    behind = passed = 0
    for p, n in order:
        for h in (0, 1):
            if n == (1 if p else 3):
                first_relay(p, h).wait_recv()
            for sign, q in sends(p, n).items():
                row_hop(p, h, q, sign).start()
        behind += SIZES[p]
        while behind - SIZES[order[passed][0]] >= LAG:
            behind -= SIZES[order[passed][0]]
            pass_on(passed)
            passed += 1
    for k in range(passed, len(order)):
        pass_on(k)

    def settle():
        for p in range(PIECES):
            for h in (0, 1):
                for sign in SIGNS:
                    first_hop(p, h, sign).wait_send()
                    for q in range(4):
                        row_hop(p, h, q, sign).wait_send()
                first_relay(p, h).wait_send()
                for q in range(4):
                    row_relay(p, h, q).wait_send()
                for part in (0, 1):
                    share(p, h, part).wait_send()

    for _, p, stage in due:
        stage(p)
        if p == PIECES - 1 and stage is other_groups:
            settle()
    for p in range(PIECES):
        for name in names:
            leaf(p, name).wait_send()


def on_device(activations, grad_output, holder_index, row_offset, column_offset, live_counts):
    tokens, slots = activations.shape[0], row_offset.shape[1]
    dma = pltpu.SemaphoreType.DMA
    out = pl.pallas_call(
        kernel,
        out_shape=pltpu.VMEM((slots // RING, BLK, BLK), jnp.float32),
        in_specs=[pl.BlockSpec(memory_space=pl.ANY)] * 6,
        out_specs=pl.BlockSpec(memory_space=pltpu.VMEM),
        scratch_shapes=[pltpu.VMEM((64, size, tokens), jnp.bfloat16) for size in SIZES]
        + [pltpu.VMEM((RING, 4, size, BLK), jnp.float32) for size in SIZES]
        + [pltpu.VMEM((7, 4, size, BLK), jnp.float32) for size in SIZES]
        + [
            pltpu.SMEM((1, slots), jnp.int32),
            pltpu.SMEM(row_offset.shape, jnp.int32),
            pltpu.SMEM(row_offset.shape, jnp.int32),
            pltpu.SMEM(live_counts.shape, jnp.int32),
            pltpu.SMEM((slots,), jnp.int32),
            dma((4,)),
            pltpu.VMEM(activations.shape, jnp.bfloat16),
            pltpu.VMEM(grad_output.shape, jnp.bfloat16),
            pltpu.VMEM((8 * max(SIZES), tokens), jnp.bfloat16),
            dma,
            dma,
        ]
        + [dma((PIECES, 2, 2))] * 2
        + [dma((PIECES, 2))] * 2
        + [dma((PIECES, 2, 4, 2))] * 2
        + [dma((PIECES, 2, 4))] * 2
        + [dma((PIECES, 2, 2))] * 2
        + [dma((PIECES, 8))] * 2,
        compiler_params=pltpu.CompilerParams(
            collective_id=0, has_side_effects=True, vmem_limit_bytes=56 * 1024 * 1024
        ),
    )(holder_index.transpose(0, 2, 1), row_offset, column_offset, live_counts, activations, grad_output)
    return out[None]


def solution(mesh):
    placed = (P("dp", "mp"), P("dp", "mp"), P(), P(), P(), P())
    return jax.shard_map(
        on_device, mesh=mesh, in_specs=placed, out_specs=P("mp", "dp", None, None), check_vma=False
    )
```
